8 devices in a mesh: dp: 2 (over z, y), cp: 4 (over x, core).
Axes of the slice: x: 2, y: 2, z: 1, core: 2. Of those that a mesh axis runs over, the one named last changes fastest.
Arguments:
- hidden: bfloat16 [32, 512, 3584], P('dp', 'cp'), parts along dimension 0
- positions: int32 [32, 512], P('dp', 'cp'), parts along dimension 0
- norm_gain: bfloat16 [3584], replicated
- w_query: bfloat16 [3584, 3584], replicated
- w_key: bfloat16 [3584, 512], replicated
- w_value: bfloat16 [3584, 512], replicated
- w_out: bfloat16 [28, 128, 3584], replicated
Outputs:
- output: bfloat16 [32, 512, 3584], P('dp', 'cp'), parts along dimension 0
There are 2 independent parts. The reference program is written for one: setup_inputs(seed, part) draws one part's arguments, and reference() takes and returns one part's arrays. A program takes and returns all parts, laid end to end along the dimension named above; an argument that names none is the same for every part.
All inputs are finite; a program needn't handle non-finite values.
Results may differ from the reference program's by a relative error of at most 0.0074385.
Values are sent between devices in bfloat16 or wider.
A program may use at most 1 GiB of HBM per device.

```python
import jax
import jax.numpy as jnp
from jax import lax

BATCH = 16
SEQ = 512
QBLOCK = 128
D = 3584
HEADS = 28
KV_HEADS = 4
HEAD = 128

GROUPS = HEADS // KV_HEADS
NBLOCKS = SEQ // QBLOCK


def draw_positions(pos_key):
    off_key, stride_key = jax.random.split(pos_key)
    offsets = jax.random.randint(off_key, (BATCH, 1), 0, SEQ)
    strides = jax.random.randint(stride_key, (BATCH, SEQ), 1, 3)
    return (offsets + jnp.cumsum(strides, axis=1) - 1).astype(jnp.int32)


def normal_weight(weight_key, shape, scale):
    return (scale * jax.random.normal(weight_key, shape, jnp.float32)).astype(jnp.bfloat16)


def setup_inputs(seed: int = 0, part: int = 0) -> dict:
    root = jax.random.key(seed)
    part_key = jax.random.fold_in(root, part)
    shared = jax.random.fold_in(root, 1000003)
    hid_key, pos_key = jax.random.split(part_key)
    gain_key, q_key, k_key, v_key, o_key = jax.random.split(shared, 5)
    hidden = (0.25 * jax.random.normal(hid_key, (BATCH, SEQ, D), jnp.float32)).astype(jnp.bfloat16)
    norm_gain = (1.0 + 0.3 * jax.random.normal(gain_key, (D,), jnp.float32)).astype(jnp.bfloat16)
    return {
        'hidden': hidden,
        'positions': draw_positions(pos_key),
        'norm_gain': norm_gain,
        'w_query': normal_weight(q_key, (D, HEADS * HEAD), 1.3 * D ** -0.5),
        'w_key': normal_weight(k_key, (D, KV_HEADS * HEAD), 1.3 * D ** -0.5),
        'w_value': normal_weight(v_key, (D, KV_HEADS * HEAD), D ** -0.5),
        'w_out': normal_weight(o_key, (HEADS, HEAD, D), 2.0 * (HEADS * HEAD) ** -0.5),
    }


def rms_norm(hidden, norm_gain):
    x_f32 = hidden.astype(jnp.float32)
    inv_rms = lax.rsqrt(jnp.mean(x_f32 * x_f32, axis=-1, keepdims=True) + 1e-5)
    return (x_f32 * inv_rms * norm_gain.astype(jnp.float32)).astype(jnp.bfloat16)


def rotary(proj_f32, positions):
    head_dim = proj_f32.shape[-1]
    half_dim = head_dim // 2
    inv_freq = 10000.0 ** (-2.0 * jnp.arange(half_dim, dtype=jnp.float32) / head_dim)
    angles = positions.astype(jnp.float32)[:, :, None] * inv_freq
    cos_part = jnp.cos(angles)[:, :, None, :]
    sin_part = jnp.sin(angles)[:, :, None, :]
    first_half = proj_f32[..., :half_dim]
    second_half = proj_f32[..., half_dim:]
    return jnp.concatenate([first_half * cos_part - second_half * sin_part, second_half * cos_part + first_half * sin_part], axis=-1).astype(jnp.bfloat16)


def reference(hidden, positions, norm_gain, w_query, w_key, w_value, w_out):
    normed = rms_norm(hidden, norm_gain).reshape(BATCH * SEQ, D)
    q_rot = rotary(jnp.dot(normed, w_query, preferred_element_type=jnp.float32).reshape(BATCH, SEQ, HEADS, HEAD), positions)
    k_rot = rotary(jnp.dot(normed, w_key, preferred_element_type=jnp.float32).reshape(BATCH, SEQ, KV_HEADS, HEAD), positions)
    v_all = jnp.dot(normed, w_value, preferred_element_type=jnp.float32).astype(jnp.bfloat16).reshape(BATCH, SEQ, KV_HEADS, HEAD)
    q_grp = q_rot.reshape(BATCH, SEQ, KV_HEADS, GROUPS, HEAD).astype(jnp.float32)
    k_f32 = k_rot.astype(jnp.float32)
    v_f32 = v_all.astype(jnp.float32)
    w_out_grp = w_out.reshape(KV_HEADS, GROUPS, HEAD, D).astype(jnp.float32)
    token_idx = jnp.arange(QBLOCK)

    def query_block(query_idx):
        q_blk = lax.dynamic_slice_in_dim(q_grp, query_idx * QBLOCK, QBLOCK, axis=1)

        def key_step(att_state, key_idx):
            def consume(state_in):
                run_max, run_sum, acc_out = state_in
                k_blk = lax.dynamic_slice_in_dim(k_f32, key_idx * QBLOCK, QBLOCK, axis=1)
                v_blk = lax.dynamic_slice_in_dim(v_f32, key_idx * QBLOCK, QBLOCK, axis=1)
                scores = jnp.einsum('bqkgd,bskd->bkgqs', q_blk, k_blk) * (HEAD ** -0.5)
                allowed = (query_idx * QBLOCK + token_idx)[:, None] >= (key_idx * QBLOCK + token_idx)[None, :]
                scores = jnp.where(allowed, scores, -jnp.inf)
                new_max = jnp.maximum(run_max, jnp.max(scores, axis=-1))
                prob_blk = jnp.exp(scores - new_max[..., None])
                rescale = jnp.exp(run_max - new_max)
                new_sum = run_sum * rescale + jnp.sum(prob_blk, axis=-1)
                new_acc = acc_out * rescale[..., None] + jnp.einsum('bkgqs,bskd->bkgqd', prob_blk, v_blk)
                return new_max, new_sum, new_acc
            return lax.cond(key_idx <= query_idx, consume, lambda state_kept: state_kept, att_state), None

        start_state = (
            jnp.full((BATCH, KV_HEADS, GROUPS, QBLOCK), -jnp.inf, jnp.float32),
            jnp.zeros((BATCH, KV_HEADS, GROUPS, QBLOCK), jnp.float32),
            jnp.zeros((BATCH, KV_HEADS, GROUPS, QBLOCK, HEAD), jnp.float32),
        )
        final_state, _ = lax.scan(key_step, start_state, jnp.arange(NBLOCKS))
        attn_out = (final_state[2] / final_state[1][..., None]).astype(jnp.bfloat16).astype(jnp.float32)
        x_blk = lax.dynamic_slice_in_dim(hidden, query_idx * QBLOCK, QBLOCK, axis=1).astype(jnp.float32)
        return (x_blk + jnp.einsum('bkgqd,kgde->bqe', attn_out, w_out_grp)).astype(jnp.bfloat16)

    out_blocks = lax.map(query_block, jnp.arange(NBLOCKS))
    return jnp.moveaxis(out_blocks, 0, 1).reshape(BATCH, SEQ, D)
```

```python
import functools

import jax
import jax.numpy as jnp
from jax import lax
from jax.experimental import pallas as pl
from jax.experimental.pallas import tpu as pltpu
from jax.sharding import PartitionSpec as P

BF = jnp.bfloat16
F32 = jnp.float32
HD = 128
VMEM_LIMIT = 60 * 1024 * 1024


def rope_tile(acc, cos, sin):
    return acc * cos + pltpu.roll(acc, HD // 2, 1) * sin


def kv_kernel(n_kv, x_ref, g_ref, wk_ref, wv_ref, cos_ref, sin_ref, kv_ref, h_ref):
    nb, seq, dim = x_ref.shape
    x = x_ref[...].reshape(nb * seq, dim).astype(F32)
    inv = lax.rsqrt(jnp.mean(x * x, axis=-1, keepdims=True) + 1e-5)
    h = (x * inv * g_ref[...].astype(F32)).astype(BF)
    h_ref[...] = h
    cos, sin = cos_ref[...], sin_ref[...]
    k = jnp.dot(h, wk_ref[...], preferred_element_type=F32)
    for n in range(n_kv):
        kv_ref[:, n, :, :] = rope_tile(k[:, n * HD:(n + 1) * HD], cos, sin).astype(BF).reshape(nb, seq, HD)
    v = jnp.dot(h, wv_ref[...], preferred_element_type=F32).astype(BF)
    for n in range(n_kv):
        kv_ref[:, n_kv + n, :, :] = v[:, n * HD:(n + 1) * HD].reshape(nb, seq, HD)


def kv_proj(x, g, wk, wv, cos, sin, b0, nbatch, nb=2):
    _, seq, dim = x.shape
    kvw = wk.shape[1]
    n_kv = kvw // HD
    rows = nb * seq
    o = b0 // nb
    return pl.pallas_call(
        functools.partial(kv_kernel, n_kv), grid=(nbatch // nb,),
        in_specs=[
            pl.BlockSpec((nb, seq, dim), lambda i: (i + o, 0, 0)),
            pl.BlockSpec((1, dim), lambda i: (0, 0)),
            pl.BlockSpec((dim, kvw), lambda i: (0, 0)),
            pl.BlockSpec((dim, kvw), lambda i: (0, 0)),
            pl.BlockSpec((rows, HD), lambda i: (i + o, 0)),
            pl.BlockSpec((rows, HD), lambda i: (i + o, 0)),
        ],
        out_specs=[
            pl.BlockSpec((nb, 2 * n_kv, seq, HD), lambda i: (i, 0, 0, 0)),
            pl.BlockSpec((rows, dim), lambda i: (i, 0)),
        ],
        out_shape=[
            jax.ShapeDtypeStruct((nbatch, 2 * n_kv, seq, HD), BF),
            jax.ShapeDtypeStruct((nbatch * seq, dim), BF),
        ],
        compiler_params=pltpu.CompilerParams(vmem_limit_bytes=VMEM_LIMIT),
        cost_estimate=pl.CostEstimate(flops=4 * nbatch * seq * dim * kvw, bytes_accessed=4 * nbatch * seq * dim, transcendentals=0),
        name="kv_proj",
    )(x, g, wk, wv, cos, sin)


def q_kernel(mc, ha_ref, hb_ref, w_ref, cos_ref, sin_ref, q_ref):
    n_heads = w_ref.shape[1] // HD
    nb = mc // HD
    for half, h_ref in enumerate((ha_ref, hb_ref)):
        base = half * ha_ref.shape[0]

        def body(i):
            r = pl.multiple_of(i * mc, mc)
            acc = jnp.dot(h_ref[pl.ds(r, mc), :], w_ref[...], preferred_element_type=F32)
            rr = pl.multiple_of(base + i * mc, mc)
            cos, sin = cos_ref[pl.ds(rr, mc), :], sin_ref[pl.ds(rr, mc), :]
            for n in range(n_heads):
                t = rope_tile(acc[:, n * HD:(n + 1) * HD], cos, sin).astype(BF)
                q_ref[pl.ds(base // HD + i * nb, nb), n, :, :] = t.reshape(nb, HD, HD)

        pl.loop(0, h_ref.shape[0] // mc)(body)


def q_proj(ha, hb, w, cos, sin, tn=512, mc=1024):
    rows = ha.shape[0] + hb.shape[0]
    dim, width = w.shape
    batch = rows // HD
    return pl.pallas_call(
        functools.partial(q_kernel, mc), grid=(width // tn,),
        in_specs=[
            pl.BlockSpec(ha.shape, lambda j: (0, 0)),
            pl.BlockSpec(hb.shape, lambda j: (0, 0)),
            pl.BlockSpec((dim, tn), lambda j: (0, j)),
            pl.BlockSpec((rows, HD), lambda j: (0, 0)),
            pl.BlockSpec((rows, HD), lambda j: (0, 0)),
        ],
        out_specs=pl.BlockSpec((batch, tn // HD, HD, HD), lambda j: (0, j, 0, 0)),
        out_shape=jax.ShapeDtypeStruct((batch, width // HD, HD, HD), BF),
        compiler_params=pltpu.CompilerParams(vmem_limit_bytes=VMEM_LIMIT),
        cost_estimate=pl.CostEstimate(flops=2 * rows * dim * width, bytes_accessed=4 * rows * dim, transcendentals=0),
        name="q_proj",
    )(ha, hb, w, cos, sin)


SCALE = 1.4426950408889634 * HD ** -0.5


def attend_heads(n_blocks, n_kv, groups, q_ref, kv_refs, o_ref):
    row = lax.broadcasted_iota(jnp.int32, (HD, HD), 0)
    col = lax.broadcasted_iota(jnp.int32, (HD, HD), 1)
    bias = jnp.where(row >= col, 0.0, -jnp.inf).astype(F32)
    for u in range(n_kv):
        k = jnp.concatenate([r[0, u] for r in kv_refs[:n_blocks]], 0)
        v = jnp.concatenate([r[0, n_kv + u] for r in kv_refs[:n_blocks]], 0).astype(F32)
        q = q_ref[0, u * groups:(u + 1) * groups].reshape(groups * HD, HD)
        scores = lax.dot_general(q, k, (((1,), (1,)), ((), ())), preferred_element_type=F32)
        for n in range(groups):
            s = scores[n * HD:(n + 1) * HD]
            s_diag = s[:, :HD] + bias
            s = s_diag if n_blocks == 1 else jnp.concatenate([s_diag, s[:, HD:]], 1)
            m = jnp.max(s, axis=-1, keepdims=True)
            p = jnp.exp2(s * SCALE - m * SCALE)
            total = jnp.sum(p, axis=-1, keepdims=True)
            acc = jnp.dot(p, v, preferred_element_type=F32)
            head = u * groups + n
            o_ref[0, :, head * HD:(head + 1) * HD] = (acc / total).astype(BF)


def attn_kernel(n_kv, groups, n_cp, q_ref, own_ref, r1_ref, r2_ref, r3_ref, o_ref):
    me = lax.axis_index("cp")
    plans = ((own_ref,), (own_ref, r2_ref), (own_ref, r1_ref, r3_ref), (own_ref, r1_ref, r2_ref, r3_ref))
    for c in range(n_cp):
        @pl.when(me == c)
        def _(c=c):
            attend_heads(c + 1, n_kv, groups, q_ref, plans[c], o_ref)


def attention(q, own, r1, r2, r3, b0, n_cp):
    batch, n2, seq, hd = own.shape
    heads = q.shape[1]
    n_kv = n2 // 2
    kv_spec = pl.BlockSpec((1, n2, seq, hd), lambda b: (b, 0, 0, 0))
    return pl.pallas_call(
        functools.partial(attn_kernel, n_kv, heads // n_kv, n_cp), grid=(batch,),
        in_specs=[pl.BlockSpec((1, heads, seq, hd), lambda b: (b + b0, 0, 0, 0)), kv_spec, kv_spec, kv_spec, kv_spec],
        out_specs=pl.BlockSpec((1, seq, heads * hd), lambda b: (b, 0, 0)),
        out_shape=jax.ShapeDtypeStruct((batch, seq, heads * hd), BF),
        compiler_params=pltpu.CompilerParams(vmem_limit_bytes=VMEM_LIMIT),
        cost_estimate=pl.CostEstimate(flops=16 * batch * heads * seq * seq * hd * 2, bytes_accessed=4 * batch * heads * seq * hd, transcendentals=0),
        name="attention",
    )(q, own, r1, r2, r3)


def out_kernel(mc, aliased, o_ref, w_ref, x_ref, *rest):
    y_ref = rest[-1]
    tn = w_ref.shape[1]
    nb = mc // HD

    def body(i):
        r = pl.multiple_of(i * mc, mc)
        acc = jnp.dot(o_ref[pl.ds(r, mc), :], w_ref[...], preferred_element_type=F32)
        b = pl.ds(i * nb, nb)
        y_ref[b] = (x_ref[b].astype(F32) + acc.reshape(nb, HD, tn)).astype(BF)

    pl.loop(0, o_ref.shape[0] // mc)(body)


def out_proj(o, w, x, b0, y_prev=None, tn=512, mc=1024):
    rows, dim = o.shape
    width = w.shape[1]
    batch = rows // HD
    spec = pl.BlockSpec((batch, HD, tn), lambda j: (b0 // batch, 0, j))
    args = [o, w, x]
    in_specs = [pl.BlockSpec((rows, dim), lambda j: (0, 0)), pl.BlockSpec((dim, tn), lambda j: (0, j)), spec]
    if y_prev is not None:
        args.append(y_prev)
        in_specs.append(pl.BlockSpec(memory_space=pl.ANY))
    return pl.pallas_call(
        functools.partial(out_kernel, mc, y_prev is not None), grid=(width // tn,),
        in_specs=in_specs, out_specs=spec,
        out_shape=jax.ShapeDtypeStruct(x.shape, BF),
        input_output_aliases={} if y_prev is None else {3: 0},
        compiler_params=pltpu.CompilerParams(vmem_limit_bytes=VMEM_LIMIT),
        cost_estimate=pl.CostEstimate(flops=2 * rows * dim * width, bytes_accessed=4 * rows * dim, transcendentals=0),
        name="out_proj",
    )(*args)


def rope_tables(positions):
    half = HD // 2
    inv_freq = 10000.0 ** (-2.0 * jnp.arange(half, dtype=F32) / HD)
    angles = positions.reshape(-1, 1).astype(F32) * inv_freq
    cos, sin = jnp.cos(angles), jnp.sin(angles)
    return jnp.concatenate([cos, cos], 1), jnp.concatenate([-sin, sin], 1)


def solution(mesh):
    n_cp = mesh.shape['cp']

    def local_block(hidden, positions, norm_gain, w_query, w_key, w_value, w_out):
        batch, seq, dim = hidden.shape
        heads = w_out.shape[0]
        half = batch // 2
        gain = norm_gain.reshape(1, dim)
        cos, sin = rope_tables(positions)
        own, h = [], []
        for i in range(2):
            kv_i, h_i = kv_proj(hidden, gain, w_key, w_value, cos, sin, i * half, half)
            own.append(kv_i)
            h.append(h_i)
        r1 = [lax.ppermute(t, 'cp', [(0, 2), (1, 3)]) for t in own]
        r2 = [lax.ppermute(t, 'cp', [(0, 1), (2, 3)]) for t in own]
        r3 = [lax.ppermute(t, 'cp', [(2, 3), (3, 2)]) for t in r1]
        q = q_proj(h[0], h[1], w_query, cos, sin)
        y = None
        w_flat = w_out.reshape(heads * HD, dim)
        for i in range(2):
            o = attention(q, own[i], r1[i], r2[i], r3[i], i * half, n_cp)
            y = out_proj(o.reshape(half * seq, heads * HD), w_flat, hidden, i * half, y)
        return y

    act_spec = P('dp', 'cp', None)
    return jax.shard_map(local_block, mesh=mesh, in_specs=(act_spec, P('dp', 'cp'), P(), P(), P(), P(), P()), out_specs=act_spec, check_vma=False)
```

```python
import functools

import jax
import jax.numpy as jnp
import numpy as np
from jax import lax
from jax.experimental import pallas as pl
from jax.experimental.pallas import tpu as pltpu
from jax.sharding import PartitionSpec as P

BF = jnp.bfloat16
F32 = jnp.float32
HD = 128
TN = 512
VMEM_LIMIT = 67043328
SCALE = 1.4426950408889634 * HD ** -0.5


def cdot(a, b):
    return jnp.dot(a, b, preferred_element_type=F32)


def rope_tile(acc, cos, sin):
    return acc * cos + pltpu.roll(acc, HD // 2, 1) * sin


def sin_cos(angle):
    n = jnp.floor(angle * 0.6366197723675814 + 0.5)
    r = angle - n * 1.5703125
    r = r - n * 4.837512969970703e-4
    r = r - n * 7.549790126404332e-08
    r2 = r * r
    s = r + r * r2 * (-1.6666654611e-1 + r2 * (8.3321608736e-3 + r2 * -1.9515295891e-4))
    c = 1.0 - 0.5 * r2 + r2 * r2 * (4.166664568298827e-2 + r2 * (-1.388731625493765e-3 + r2 * 2.443315711809948e-5))
    q = n.astype(jnp.int32)
    odd = (q & 1) == 1
    sin_v = jnp.where(odd, c, s)
    cos_v = jnp.where(odd, s, c)
    sin_v = jnp.where((q & 2) == 2, -sin_v, sin_v)
    cos_v = jnp.where(((q + 1) & 2) == 2, -cos_v, cos_v)
    return sin_v, cos_v


def attend_heads(n_blocks, n_kv, groups, q_ref, kv_refs, o_ref):
    row = lax.broadcasted_iota(jnp.int32, (HD, HD), 0)
    col = lax.broadcasted_iota(jnp.int32, (HD, HD), 1)
    bias = jnp.where(row >= col, 0.0, -jnp.inf).astype(F32)
    for u in range(n_kv):
        k = jnp.concatenate([r[u] for r in kv_refs[:n_blocks]], 0)
        v = jnp.concatenate([r[n_kv + u] for r in kv_refs[:n_blocks]], 0).astype(F32)
        q = q_ref[u * groups:(u + 1) * groups].reshape(groups * HD, HD)
        scores = lax.dot_general(q, k, (((1,), (1,)), ((), ())), preferred_element_type=F32)
        for n in range(groups):
            s = scores[n * HD:(n + 1) * HD]
            s_diag = s[:, :HD] + bias
            s = s_diag if n_blocks == 1 else jnp.concatenate([s_diag, s[:, HD:]], 1)
            m = jnp.max(s, axis=-1, keepdims=True)
            p = jnp.exp2(s * SCALE - m * SCALE)
            total = jnp.sum(p, axis=-1, keepdims=True)
            head = u * groups + n
            o_ref[:, head * HD:(head + 1) * HD] = (cdot(p, v) / total).astype(BF)


def attend_any(me, n_cp, n_kv, groups, q_ref, own, r1, r2, r3, o_ref):
    plans = ((own,), (own, r2), (own, r1, r3), (own, r1, r2, r3))
    for c in range(n_cp):
        @pl.when(me == c)
        def _(c=c):
            attend_heads(c + 1, n_kv, groups, q_ref, plans[c], o_ref)


def front_kernel(n_kv, n_first, forward_q, forward_a,
                 x_hbm, pos_ref, gain_ref, freq_ref, wq_hbm, wk_hbm, wv_hbm,
                 q_hbm, o_hbm, own_hbm, r1_hbm, r2_hbm, r3_hbm,
                 h_ref, kv_ref, cos_ref, sin_ref, x_buf, w_buf, q_buf, qa_buf, ra_buf, oa_buf,
                 x_sem, w_sem, q_sem, qa_sem, ra_sem, oa_sem, own_sem,
                 send1, recv1, send2, recv2, send3, recv3):
    batch, seq, dim = x_hbm.shape
    heads = q_hbm.shape[1]
    groups = heads // n_kv
    nb = x_buf.shape[1]
    n_chunks = batch // nb
    rows = nb * seq
    n_tiles = wq_hbm.shape[1] // TN
    tile_heads = TN // HD
    me = lax.axis_index("cp")
    low, high, odd = me < 2, me >= 2, lax.rem(me, 2) == 1

    def x_copy(i):
        s = lax.rem(i, 2)
        return pltpu.make_async_copy(x_hbm.at[pl.ds(i * nb, nb)], x_buf.at[s], x_sem.at[s])

    def wq_copy(j):
        s = lax.rem(j + 2, 3)
        return pltpu.make_async_copy(wq_hbm.at[:, pl.ds(pl.multiple_of(j * TN, TN), TN)], w_buf.at[s], w_sem.at[s])

    wk_copy = pltpu.make_async_copy(wk_hbm, w_buf.at[0], w_sem.at[0])
    wv_copy = pltpu.make_async_copy(wv_hbm, w_buf.at[1], w_sem.at[1])
    x_copy(0).start()
    wk_copy.start()
    wv_copy.start()
    x_copy(1).start()
    wq_copy(0).start()

    def part(ref, i):
        return ref.at[pl.ds(i * nb, nb)]

    def remote(src, dst, i, send, recv, target):
        return pltpu.make_async_remote_copy(
            src_ref=part(src, i), dst_ref=part(dst, i), send_sem=send.at[i], recv_sem=recv.at[i],
            device_id={"cp": target}, device_id_type=pl.DeviceIdType.MESH)

    def copy1(i):
        return remote(kv_ref, r1_hbm, i, send1, recv1, lax.rem(me + 2, 4))

    def copy2(i):
        return remote(kv_ref, r2_hbm, i, send2, recv2, me + 1 - 2 * lax.rem(me, 2))

    def copy3(i):
        return remote(r1_hbm, r3_hbm, i, send3, recv3, me + 1 - 2 * lax.rem(me, 2))

    lane = lax.broadcasted_iota(jnp.int32, (1, HD), 1)
    sign = jnp.where(lane < HD // 2, -1.0, 1.0).astype(F32)

    def table(b):
        pos = jnp.broadcast_to(pos_ref[pl.ds(b, 1), :].astype(F32), (HD, HD)).T
        s, c = sin_cos(pos * freq_ref[...])
        at = pl.ds(pl.multiple_of(b * HD, HD), HD)
        cos_ref[at, :] = c
        sin_ref[at, :] = s * sign

    pl.loop(0, batch)(table)

    barrier = pltpu.get_barrier_semaphore()
    for target in (lax.rem(me + 2, 4), me + 1 - 2 * lax.rem(me, 2)):
        pl.semaphore_signal(barrier, inc=1, device_id={"cp": target}, device_id_type=pl.DeviceIdType.MESH)
    pl.semaphore_wait(barrier, 2)

    def send(i):
        @pl.when(low)
        def _():
            copy1(i).start()

        @pl.when(jnp.logical_not(odd))
        def _():
            copy2(i).start()

    wk_copy.wait()
    wv_copy.wait()

    def kv_chunk(i):
        x_copy(i).wait()
        at = pl.ds(pl.multiple_of(i * rows, rows), rows)
        x = x_buf[lax.rem(i, 2)].reshape(rows, dim).astype(F32)
        inv = lax.rsqrt(jnp.mean(x * x, axis=-1, keepdims=True) + 1e-5)
        h = (x * inv * gain_ref[...].astype(F32)).astype(BF)
        h_ref[at, :] = h
        cos, sin = cos_ref[at, :], sin_ref[at, :]
        k = cdot(h, w_buf[0])
        to = pl.ds(i * nb, nb)
        for n in range(n_kv):
            kv_ref[to, n] = rope_tile(k[:, n * HD:(n + 1) * HD], cos, sin).astype(BF).reshape(nb, seq, HD)
        v = cdot(h, w_buf[1]).astype(BF)
        for n in range(n_kv):
            kv_ref[to, n_kv + n] = v[:, n * HD:(n + 1) * HD].reshape(nb, seq, HD)

        @pl.when(i + 2 < n_chunks)
        def _():
            x_copy(i + 2).start()

        @pl.when(i > 0)
        def _():
            send(i - 1)

    pl.loop(0, n_chunks)(kv_chunk)
    wq_copy(1).start()

    def forward(i):
        @pl.when(high)
        def _():
            copy1(i).wait_recv()
            copy3(i).start()

    def q_copy(j):
        s = lax.rem(j, 2)
        return pltpu.make_async_copy(q_buf.at[s], q_hbm.at[:, pl.ds(j * tile_heads, tile_heads)], q_sem.at[s])

    own_copy = pltpu.make_async_copy(kv_ref.at[pl.ds(n_first, batch - n_first)], own_hbm, own_sem)
    mc = 1024

    def q_tile(j):
        @pl.when(j == 0)
        def _():
            send(n_chunks - 1)
            own_copy.start()

        for at, chunk in forward_q:
            @pl.when(j == at)
            def _(chunk=chunk):
                forward(chunk)

        wq_copy(j).wait()

        @pl.when(jnp.logical_and(j > 0, j + 1 < n_tiles))
        def _():
            wq_copy(j + 1).start()

        @pl.when(j >= 2)
        def _():
            q_copy(j - 2).wait()

        ws, qs = lax.rem(j + 2, 3), lax.rem(j, 2)

        def rows_step(i):
            at = pl.ds(pl.multiple_of(i * mc, mc), mc)
            acc = cdot(h_ref[at, :], w_buf[ws])
            cos, sin = cos_ref[at, :], sin_ref[at, :]
            for n in range(tile_heads):
                t = rope_tile(acc[:, n * HD:(n + 1) * HD], cos, sin).astype(BF)
                q_buf[qs, pl.ds(i * (mc // HD), mc // HD), n] = t.reshape(mc // HD, HD, HD)

        pl.loop(0, batch * seq // mc)(rows_step)
        q_copy(j).start()

    pl.loop(0, n_tiles)(q_tile)
    q_copy(n_tiles - 2).wait()
    q_copy(n_tiles - 1).wait()

    first_chunks = n_first // nb
    for i in range(first_chunks):
        @pl.when(odd)
        def _(i=i):
            copy2(i).wait_recv()

        @pl.when(high)
        def _(i=i):
            copy3(i).wait_recv()

    def loads(b):
        s = lax.rem(b, 2)
        pairs = [(None, pltpu.make_async_copy(q_hbm.at[b], qa_buf.at[s], qa_sem.at[s]))]
        for n, (ref, used) in enumerate(((r1_hbm, high), (r2_hbm, odd), (r3_hbm, high))):
            pairs.append((used, pltpu.make_async_copy(ref.at[b], ra_buf.at[s, n], ra_sem.at[s, n])))
        return pairs

    def start_loads(b):
        for used, copy in loads(b):
            if used is None:
                copy.start()
            else:
                pl.when(used)(copy.start)

    def wait_loads(b):
        for used, copy in loads(b):
            if used is None:
                copy.wait()
            else:
                pl.when(used)(copy.wait)

    def o_copy(b):
        s = lax.rem(b, 2)
        return pltpu.make_async_copy(oa_buf.at[s], o_hbm.at[pl.ds(pl.multiple_of(b * seq, seq), seq)], oa_sem.at[s])

    start_loads(0)

    def attend(b):
        for at, chunk in forward_a:
            @pl.when(b == at)
            def _(chunk=chunk):
                forward(chunk)

        wait_loads(b)

        @pl.when(b + 1 < n_first)
        def _():
            start_loads(b + 1)

        @pl.when(b >= 2)
        def _():
            o_copy(b - 2).wait()

        s = lax.rem(b, 2)
        attend_any(me, 4, n_kv, groups, qa_buf.at[s], kv_ref.at[b], ra_buf.at[s, 0], ra_buf.at[s, 1], ra_buf.at[s, 2], oa_buf.at[s])
        o_copy(b).start()

    pl.loop(0, n_first)(attend)
    o_copy(n_first - 2).wait()
    o_copy(n_first - 1).wait()
    own_copy.wait()
    done = [c for _, c in forward_q] + [c for _, c in forward_a]
    for i in range(n_chunks):
        if i not in done:
            forward(i)
    for i in range(n_chunks):
        @pl.when(low)
        def _(i=i):
            copy1(i).wait_send()

        @pl.when(jnp.logical_not(odd))
        def _(i=i):
            copy2(i).wait_send()

        @pl.when(high)
        def _(i=i):
            copy3(i).wait_send()

        if i >= first_chunks:
            @pl.when(odd)
            def _(i=i):
                copy2(i).wait_recv()

            @pl.when(high)
            def _(i=i):
                copy3(i).wait_recv()


def back_kernel(n_kv, n_first, q_hbm, oa_hbm, own_hbm, r1_hbm, r2_hbm, r3_hbm, w_hbm, x_hbm,
                y_hbm, o_ref, w_buf, x_buf, y_buf, q_buf, kv_buf,
                o_sem, w_sem, x_sem, y_sem, q_sem, kv_sem):
    batch, seq, dim = x_hbm.shape
    half = batch - n_first
    heads = q_hbm.shape[1]
    groups = heads // n_kv
    n_tiles = dim // TN
    me = lax.axis_index("cp")
    high, odd = me >= 2, lax.rem(me, 2) == 1

    def w_copy(t):
        s = lax.rem(t, 2)
        col = pl.multiple_of(lax.rem(t, n_tiles) * TN, TN)
        return pltpu.make_async_copy(w_hbm.at[:, pl.ds(col, TN)], w_buf.at[s], w_sem.at[s])

    def x_copy(t):
        s = lax.rem(t, 2)
        col = pl.multiple_of(lax.rem(t, n_tiles) * TN, TN)
        return pltpu.make_async_copy(x_hbm.at[pl.ds(lax.div(t, n_tiles) * half, half), :, pl.ds(col, TN)], x_buf.at[s], x_sem.at[s])

    def y_copy(t):
        s = lax.rem(t, 2)
        col = pl.multiple_of(lax.rem(t, n_tiles) * TN, TN)
        return pltpu.make_async_copy(y_buf.at[s], y_hbm.at[pl.ds(lax.div(t, n_tiles) * half, half), :, pl.ds(col, TN)], y_sem.at[s])

    def loads(b):
        s = lax.rem(b, 2)
        pairs = [(None, pltpu.make_async_copy(q_hbm.at[n_first + b], q_buf.at[s], q_sem.at[s]))]
        for n, (ref, used, at) in enumerate(((own_hbm, None, b), (r1_hbm, high, n_first + b), (r2_hbm, odd, n_first + b), (r3_hbm, high, n_first + b))):
            pairs.append((used, pltpu.make_async_copy(ref.at[at], kv_buf.at[s, n], kv_sem.at[s, n])))
        return pairs

    def run_loads(b, act):
        for used, copy in loads(b):
            if used is None:
                getattr(copy, act)()
            else:
                pl.when(used)(getattr(copy, act))

    oa_copy = pltpu.make_async_copy(oa_hbm, o_ref.at[0], o_sem)
    w_copy(0).start()
    oa_copy.start()
    x_copy(0).start()
    run_loads(0, "start")
    oa_copy.wait()
    mc = 1024

    def attend(b):
        run_loads(b, "wait")

        @pl.when(b + 1 < half)
        def _():
            run_loads(b + 1, "start")

        s = lax.rem(b, 2)
        attend_any(me, 4, n_kv, groups, q_buf.at[s], kv_buf.at[s, 0], kv_buf.at[s, 1], kv_buf.at[s, 2], kv_buf.at[s, 3],
                   o_ref.at[1, pl.ds(pl.multiple_of(b * seq, seq), seq)])

    def phase(p):
        @pl.when(p == 1)
        def _():
            pl.loop(0, half)(attend)

        def tile(j):
            t = p * n_tiles + j
            s = lax.rem(t, 2)
            w_copy(t).wait()
            x_copy(t).wait()

            @pl.when(t + 1 < 2 * n_tiles)
            def _():
                w_copy(t + 1).start()
                x_copy(t + 1).start()

            @pl.when(t >= 2)
            def _():
                y_copy(t - 2).wait()

            def rows_step(i):
                acc = cdot(o_ref[p, pl.ds(pl.multiple_of(i * mc, mc), mc), :], w_buf[s])
                to = pl.ds(i * (mc // HD), mc // HD)
                y_buf[s, to] = (x_buf[s, to].astype(F32) + acc.reshape(mc // HD, HD, TN)).astype(BF)

            pl.loop(0, half * seq // mc)(rows_step)
            y_copy(t).start()

        pl.loop(0, n_tiles)(tile)

    pl.loop(0, 2)(phase)
    y_copy(2 * n_tiles - 2).wait()
    y_copy(2 * n_tiles - 1).wait()


def solution(mesh):
    dma = pltpu.SemaphoreType.DMA

    def local_block(hidden, positions, norm_gain, w_query, w_key, w_value, w_out):
        batch, seq, dim = hidden.shape
        heads = w_out.shape[0]
        n_kv = w_key.shape[1] // HD
        first = batch // 2
        nb = 2
        n_chunks = batch // nb
        freq = (10000.0 ** (-2.0 * np.arange(HD // 2, dtype=np.float64) / HD)).astype(np.float32)
        freq = jnp.asarray(np.concatenate([freq, freq])[None, :])
        hbm = pl.BlockSpec(memory_space=pl.ANY)
        vmem = pl.BlockSpec(memory_space=pltpu.VMEM)
        kv_shape = (batch, 2 * n_kv, seq, HD)
        blk = (2 * n_kv, seq, HD)
        shape = jax.ShapeDtypeStruct
        forward_q = ((1, 0), (2, 1), (3, 2), (5, 3), (6, 4))
        forward_a = ((1, 5), (4, 6))
        q, o_first, own, r1, r2, r3 = pl.pallas_call(
            functools.partial(front_kernel, n_kv, first, forward_q, forward_a),
            in_specs=[hbm, vmem, vmem, vmem, hbm, hbm, hbm],
            out_specs=[hbm] * 6,
            out_shape=[
                shape((batch, heads, seq, HD), BF), shape((first * seq, heads * HD), BF),
                shape((batch - first,) + blk, BF), shape(kv_shape, BF), shape(kv_shape, BF), shape(kv_shape, BF)],
            scratch_shapes=[
                pltpu.VMEM((batch * seq, dim), BF), pltpu.VMEM(kv_shape, BF),
                pltpu.VMEM((batch * seq, HD), F32), pltpu.VMEM((batch * seq, HD), F32),
                pltpu.VMEM((2, nb, seq, dim), BF), pltpu.VMEM((3, dim, TN), BF),
                pltpu.VMEM((2, batch, TN // HD, seq, HD), BF),
                pltpu.VMEM((2, heads, seq, HD), BF), pltpu.VMEM((2, 3) + blk, BF), pltpu.VMEM((2, seq, heads * HD), BF),
                dma((2,)), dma((3,)), dma((2,)), dma((2,)), dma((2, 3)), dma((2,)), dma,
            ] + [dma((n_chunks,))] * 6,
            compiler_params=pltpu.CompilerParams(vmem_limit_bytes=VMEM_LIMIT, collective_id=0, has_side_effects=True),
            cost_estimate=pl.CostEstimate(flops=2 * batch * seq * dim * (heads + 2 * n_kv) * HD, bytes_accessed=10 * batch * seq * dim, transcendentals=0),
            name="front",
        )(hidden, positions, norm_gain.reshape(1, dim), freq, w_query, w_key, w_value)
        half = batch - first
        return pl.pallas_call(
            functools.partial(back_kernel, n_kv, first),
            in_specs=[hbm] * 8, out_specs=hbm,
            out_shape=shape((batch, seq, dim), BF),
            scratch_shapes=[
                pltpu.VMEM((2, half * seq, heads * HD), BF), pltpu.VMEM((2, heads * HD, TN), BF),
                pltpu.VMEM((2, half, seq, TN), BF), pltpu.VMEM((2, half, seq, TN), BF),
                pltpu.VMEM((2, heads, seq, HD), BF), pltpu.VMEM((2, 4) + blk, BF),
                dma, dma((2,)), dma((2,)), dma((2,)), dma((2,)), dma((2, 4)),
            ],
            compiler_params=pltpu.CompilerParams(vmem_limit_bytes=VMEM_LIMIT),
            cost_estimate=pl.CostEstimate(flops=2 * batch * seq * dim * heads * HD, bytes_accessed=10 * batch * seq * dim, transcendentals=0),
            name="back",
        )(q, o_first, own, r1, r2, r3, w_out.reshape(heads * HD, dim), hidden)

    act_spec = P('dp', 'cp', None)
    return jax.shard_map(local_block, mesh=mesh, in_specs=(act_spec, P('dp', 'cp'), P(), P(), P(), P(), P()), out_specs=act_spec, check_vma=False)
```

```python
import functools

import jax
import jax.numpy as jnp
import numpy as np
from jax import lax
from jax.experimental import pallas as pl
from jax.experimental.pallas import tpu as pltpu
from jax.sharding import PartitionSpec as P

BF = jnp.bfloat16
F32 = jnp.float32
HD = 128
TN = 512
VMEM_LIMIT = 67043328
SCALE = 1.4426950408889634 * HD ** -0.5


def cdot(a, b):
    return jnp.dot(a, b, preferred_element_type=F32)


def rope_tile(acc, cos, sin):
    return acc * cos + pltpu.roll(acc, HD // 2, 1) * sin


def sin_cos(angle):
    n = jnp.floor(angle * 0.6366197723675814 + 0.5)
    r = angle - n * 1.5703125
    r = r - n * 4.837512969970703e-4
    r = r - n * 7.549790126404332e-08
    r2 = r * r
    s = r + r * r2 * (-1.6666654611e-1 + r2 * (8.3321608736e-3 + r2 * -1.9515295891e-4))
    c = 1.0 - 0.5 * r2 + r2 * r2 * (4.166664568298827e-2 + r2 * (-1.388731625493765e-3 + r2 * 2.443315711809948e-5))
    q = n.astype(jnp.int32)
    odd = (q & 1) == 1
    sin_v = jnp.where(odd, c, s)
    cos_v = jnp.where(odd, s, c)
    sin_v = jnp.where((q & 2) == 2, -sin_v, sin_v)
    cos_v = jnp.where(((q + 1) & 2) == 2, -cos_v, cos_v)
    return sin_v, cos_v


def attend_heads(n_blocks, n_kv, groups, q_ref, kv_refs, o_ref):
    row = lax.broadcasted_iota(jnp.int32, (HD, HD), 0)
    col = lax.broadcasted_iota(jnp.int32, (HD, HD), 1)
    bias = jnp.where(row >= col, 0.0, -jnp.inf).astype(F32)
    for u in range(n_kv):
        k = jnp.concatenate([r[u] for r in kv_refs[:n_blocks]], 0)
        v = jnp.concatenate([r[n_kv + u] for r in kv_refs[:n_blocks]], 0).astype(F32)
        q = q_ref[u * groups:(u + 1) * groups].reshape(groups * HD, HD)
        scores = lax.dot_general(q, k, (((1,), (1,)), ((), ())), preferred_element_type=F32)
        for n in range(groups):
            s = scores[n * HD:(n + 1) * HD]
            s_diag = s[:, :HD] + bias
            s = s_diag if n_blocks == 1 else jnp.concatenate([s_diag, s[:, HD:]], 1)
            m = jnp.max(s, axis=-1, keepdims=True)
            p = jnp.exp2(s * SCALE - m * SCALE)
            total = jnp.sum(p, axis=-1, keepdims=True)
            head = u * groups + n
            o_ref[:, head * HD:(head + 1) * HD] = (cdot(p, v) / total).astype(BF)


def attend_any(me, n_cp, n_kv, groups, q_ref, own, r1, r2, r3, o_ref):
    plans = ((own,), (own, r2), (own, r1, r3), (own, r1, r2, r3))
    for c in range(n_cp):
        @pl.when(me == c)
        def _(c=c):
            attend_heads(c + 1, n_kv, groups, q_ref, plans[c], o_ref)


def front_kernel(n_kv, n_first, forward_q, forward_a,
                 x_hbm, pos_ref, gain_ref, freq_ref, wq_hbm, wk_hbm, wv_hbm,
                 q_hbm, o_hbm, own_hbm, r1_hbm, r2_hbm, r3_hbm,
                 h_ref, ha_ref, hb_ref, kv_ref, cos_ref, sin_ref, x_buf, w_buf, q_buf, acc_ref, qa_buf, ra_buf, oa_buf,
                 x_sem, w_sem, q_sem, qa_sem, ra_sem, oa_sem, own_sem,
                 send1, recv1, send2, recv2, send3, recv3):
    batch, seq, dim = x_hbm.shape
    heads = q_hbm.shape[1]
    groups = heads // n_kv
    nb = x_buf.shape[1]
    n_chunks = batch // nb
    rows = nb * seq
    n_tiles = wq_hbm.shape[1] // TN
    tile_heads = TN // HD
    me = lax.axis_index("cp")
    low, high, odd = me < 2, me >= 2, lax.rem(me, 2) == 1

    def x_copy(i):
        s = lax.rem(i, 2)
        return pltpu.make_async_copy(x_hbm.at[pl.ds(i * nb, nb)], x_buf.at[s], x_sem.at[s])

    def wq_copy(j):
        s = lax.rem(j + 2, 3)
        return pltpu.make_async_copy(wq_hbm.at[:, pl.ds(pl.multiple_of(j * TN, TN), TN)], w_buf.at[s], w_sem.at[s])

    wk_copy = pltpu.make_async_copy(wk_hbm, w_buf.at[0], w_sem.at[0])
    wv_copy = pltpu.make_async_copy(wv_hbm, w_buf.at[1], w_sem.at[1])
    x_copy(0).start()
    wk_copy.start()

    def part(ref, i):
        return ref.at[pl.ds(i * nb, nb)]

    def remote(src, dst, i, send, recv, target):
        return pltpu.make_async_remote_copy(
            src_ref=part(src, i), dst_ref=part(dst, i), send_sem=send.at[i], recv_sem=recv.at[i],
            device_id={"cp": target}, device_id_type=pl.DeviceIdType.MESH)

    def copy1(i):
        return remote(kv_ref, r1_hbm, i, send1, recv1, lax.rem(me + 2, 4))

    def copy2(i):
        return remote(kv_ref, r2_hbm, i, send2, recv2, me + 1 - 2 * lax.rem(me, 2))

    def copy3(i):
        return remote(r1_hbm, r3_hbm, i, send3, recv3, me + 1 - 2 * lax.rem(me, 2))

    lane = lax.broadcasted_iota(jnp.int32, (1, HD), 1)
    sign = jnp.where(lane < HD // 2, -1.0, 1.0).astype(F32)

    def table(b):
        pos = jnp.broadcast_to(pos_ref[pl.ds(b, 1), :].astype(F32), (HD, HD)).T
        s, c = sin_cos(pos * freq_ref[...])
        at = pl.ds(pl.multiple_of(b * HD, HD), HD)
        cos_ref[at, :] = c
        sin_ref[at, :] = s * sign

    pl.loop(0, batch)(table)

    barrier = pltpu.get_barrier_semaphore()
    for target in (lax.rem(me + 2, 4), me + 1 - 2 * lax.rem(me, 2)):
        pl.semaphore_signal(barrier, inc=1, device_id={"cp": target}, device_id_type=pl.DeviceIdType.MESH)

    def send(i):
        @pl.when(low)
        def _():
            copy1(i).start()

        @pl.when(jnp.logical_not(odd))
        def _():
            copy2(i).start()

    gain = jnp.concatenate([gain_ref[c:c + 1, :] for c in range(dim // HD)], 1).astype(F32)

    def norm(i, out_ref, part=0, parts=1):
        n = rows // parts
        b, r = part * n // seq, part * n % seq
        if parts == 1:
            x = x_buf[lax.rem(i, 2)].reshape(rows, dim).astype(F32)
        else:
            x = x_buf[lax.rem(i, 2), b, r:r + n].astype(F32)
        inv = lax.rsqrt(jnp.mean(x * x, axis=-1, keepdims=True) + 1e-5)
        h = (x * inv * gain).astype(BF)
        out_ref[part * n:(part + 1) * n] = h
        h_ref[pl.ds(pl.multiple_of(i * rows + part * n, n), n), :] = h

    x_copy(0).wait()
    norm(0, ha_ref)
    x_copy(1).start()
    wv_copy.start()
    x_copy(2).start()
    wk_copy.wait()
    pl.semaphore_wait(barrier, 2)
    wv_copy.wait()

    def kv_chunk(i, cur_ref, next_ref):
        @pl.when(i + 1 < n_chunks)
        def _():
            x_copy(i + 1).wait()

        at = pl.ds(pl.multiple_of(i * rows, rows), rows)
        cos, sin = cos_ref[at, :], sin_ref[at, :]
        to = pl.ds(i * nb, nb)
        parts = 4
        width = n_kv * HD
        step = 2 * width // parts
        for c in range(parts):
            col = c * step
            w = w_buf[col // width, :, col % width:col % width + step]
            acc = cdot(cur_ref[...], w)
            norm(i + 1, next_ref, c, parts)
            for n in range(step // HD):
                t = acc[:, n * HD:(n + 1) * HD]
                if col < width:
                    t = rope_tile(t, cos, sin)
                kv_ref[to, col // HD + n] = t.astype(BF).reshape(nb, seq, HD)

        @pl.when(i + 3 < n_chunks)
        def _():
            x_copy(i + 3).start()

        @pl.when(i > 0)
        def _():
            send(i - 1)

    def kv_pair(i):
        kv_chunk(2 * i, ha_ref, hb_ref)

        @pl.when(i == 0)
        def _():
            wq_copy(0).start()

        kv_chunk(2 * i + 1, hb_ref, ha_ref)

    pl.loop(0, n_chunks // 2)(kv_pair)
    wq_copy(1).start()

    def forward(i):
        @pl.when(high)
        def _():
            copy1(i).wait_recv()
            copy3(i).start()

    def q_copy(j):
        s = lax.rem(j, 3)
        return pltpu.make_async_copy(q_buf.at[s], q_hbm.at[:, pl.ds(j * tile_heads, tile_heads)], q_sem.at[s])

    own_copy = pltpu.make_async_copy(kv_ref.at[pl.ds(n_first, batch - n_first)], own_hbm, own_sem)
    mc = acc_ref.shape[1]
    n_parts = batch * seq // mc

    def finish_part(i, slot):
        at = slice(i * mc, (i + 1) * mc)
        cos, sin = cos_ref[at, :], sin_ref[at, :]
        for n in range(tile_heads):
            t = rope_tile(acc_ref[i % 2, :, n * HD:(n + 1) * HD], cos, sin).astype(BF)
            q_buf[slot, i * (mc // HD):(i + 1) * (mc // HD), n] = t.reshape(mc // HD, HD, HD)

    def q_tile(j):
        @pl.when(j == 0)
        def _():
            send(n_chunks - 1)
            own_copy.start()

        for at, chunk in forward_q:
            @pl.when(j == at)
            def _(chunk=chunk):
                forward(chunk)

        wq_copy(j).wait()

        @pl.when(jnp.logical_and(j > 0, j + 1 < n_tiles))
        def _():
            wq_copy(j + 1).start()

        @pl.when(j >= 3)
        def _():
            q_copy(j - 3).wait()

        ws, qs, before = lax.rem(j + 2, 3), lax.rem(j, 3), lax.rem(j + 2, 3)
        for i in range(n_parts):
            acc_ref[i % 2] = cdot(h_ref[i * mc:(i + 1) * mc, :], w_buf[ws])
            if i == 0:
                finish_part(n_parts - 1, before)
            else:
                finish_part(i - 1, qs)

        @pl.when(j > 0)
        def _():
            q_copy(j - 1).start()

    pl.loop(0, n_tiles)(q_tile)
    finish_part(n_parts - 1, (n_tiles - 1) % 3)
    q_copy(n_tiles - 1).start()
    for j in range(n_tiles - 3, n_tiles):
        q_copy(j).wait()

    first_chunks = n_first // nb
    for i in range(first_chunks):
        @pl.when(odd)
        def _(i=i):
            copy2(i).wait_recv()

        @pl.when(high)
        def _(i=i):
            copy3(i).wait_recv()

    def loads(b):
        s = lax.rem(b, 2)
        pairs = [(None, pltpu.make_async_copy(q_hbm.at[b], qa_buf.at[s], qa_sem.at[s]))]
        for n, (ref, used) in enumerate(((r1_hbm, high), (r2_hbm, odd), (r3_hbm, high))):
            pairs.append((used, pltpu.make_async_copy(ref.at[b], ra_buf.at[s, n], ra_sem.at[s, n])))
        return pairs

    def start_loads(b):
        for used, copy in loads(b):
            if used is None:
                copy.start()
            else:
                pl.when(used)(copy.start)

    def wait_loads(b):
        for used, copy in loads(b):
            if used is None:
                copy.wait()
            else:
                pl.when(used)(copy.wait)

    def o_copy(b):
        s = lax.rem(b, 2)
        return pltpu.make_async_copy(oa_buf.at[s], o_hbm.at[pl.ds(pl.multiple_of(b * seq, seq), seq)], oa_sem.at[s])

    start_loads(0)

    def attend(b):
        for at, chunk in forward_a:
            @pl.when(b == at)
            def _(chunk=chunk):
                forward(chunk)

        wait_loads(b)

        @pl.when(b + 1 < n_first)
        def _():
            start_loads(b + 1)

        @pl.when(b >= 2)
        def _():
            o_copy(b - 2).wait()

        s = lax.rem(b, 2)
        attend_any(me, 4, n_kv, groups, qa_buf.at[s], kv_ref.at[b], ra_buf.at[s, 0], ra_buf.at[s, 1], ra_buf.at[s, 2], oa_buf.at[s])
        o_copy(b).start()

    pl.loop(0, n_first)(attend)
    o_copy(n_first - 2).wait()
    o_copy(n_first - 1).wait()
    own_copy.wait()
    done = [c for _, c in forward_q] + [c for _, c in forward_a]
    for i in range(n_chunks):
        if i not in done:
            forward(i)
    for i in range(n_chunks):
        @pl.when(low)
        def _(i=i):
            copy1(i).wait_send()

        @pl.when(jnp.logical_not(odd))
        def _(i=i):
            copy2(i).wait_send()

        @pl.when(high)
        def _(i=i):
            copy3(i).wait_send()

        if i >= first_chunks:
            @pl.when(odd)
            def _(i=i):
                copy2(i).wait_recv()

            @pl.when(high)
            def _(i=i):
                copy3(i).wait_recv()


def back_kernel(n_kv, n_first, q_hbm, oa_hbm, own_hbm, r1_hbm, r2_hbm, r3_hbm, w_hbm, x_hbm,
                y_hbm, o_ref, w_buf, x_buf, y_buf, q_buf, kv_buf,
                o_sem, w_sem, x_sem, y_sem, q_sem, kv_sem):
    batch, seq, dim = x_hbm.shape
    half = batch - n_first
    heads = q_hbm.shape[1]
    groups = heads // n_kv
    n_tiles = dim // TN
    me = lax.axis_index("cp")
    high, odd = me >= 2, lax.rem(me, 2) == 1

    def cols(j):
        return pl.ds(pl.multiple_of(j * TN, TN), TN)

    def w_copy(j):
        s = lax.rem(j, 2)
        return pltpu.make_async_copy(w_hbm.at[:, cols(j)], w_buf.at[s], w_sem.at[s])

    def x_copy(j):
        s = lax.rem(j, 2)
        return pltpu.make_async_copy(x_hbm.at[:, :, cols(j)], x_buf.at[s], x_sem.at[s])

    def y_copy(j):
        s = lax.rem(j, 2)
        return pltpu.make_async_copy(y_buf.at[s], y_hbm.at[:, :, cols(j)], y_sem.at[s])

    def loads(b):
        s = lax.rem(b, 2)
        pairs = [(None, pltpu.make_async_copy(q_hbm.at[n_first + b], q_buf.at[s], q_sem.at[s]))]
        for n, (ref, used, at) in enumerate(((own_hbm, None, b), (r1_hbm, high, n_first + b), (r2_hbm, odd, n_first + b), (r3_hbm, high, n_first + b))):
            pairs.append((used, pltpu.make_async_copy(ref.at[at], kv_buf.at[s, n], kv_sem.at[s, n])))
        return pairs

    def run_loads(b, act):
        for used, copy in loads(b):
            if used is None:
                getattr(copy, act)()
            else:
                pl.when(used)(getattr(copy, act))

    oa_copy = pltpu.make_async_copy(oa_hbm, o_ref.at[pl.ds(0, n_first * seq)], o_sem)
    run_loads(0, "start")
    mc = 2048

    def attend(b):
        run_loads(b, "wait")

        @pl.when(b + 1 < half)
        def _():
            run_loads(b + 1, "start")

        @pl.when(b == 0)
        def _():
            oa_copy.start()
            w_copy(0).start()
            x_copy(0).start()

        s = lax.rem(b, 2)
        attend_any(me, 4, n_kv, groups, q_buf.at[s], kv_buf.at[s, 0], kv_buf.at[s, 1], kv_buf.at[s, 2], kv_buf.at[s, 3],
                   o_ref.at[pl.ds(pl.multiple_of((n_first + b) * seq, seq), seq)])

    pl.loop(0, half)(attend)
    oa_copy.wait()

    def tile(j):
        s = lax.rem(j, 2)
        w_copy(j).wait()
        x_copy(j).wait()

        @pl.when(j + 1 < n_tiles)
        def _():
            w_copy(j + 1).start()
            x_copy(j + 1).start()

        @pl.when(j >= 2)
        def _():
            y_copy(j - 2).wait()

        def rows_step(i):
            acc = cdot(o_ref[pl.ds(pl.multiple_of(i * mc, mc), mc), :], w_buf[s])
            to = pl.ds(i * (mc // HD), mc // HD)
            y_buf[s, to] = (x_buf[s, to].astype(F32) + acc.reshape(mc // HD, HD, TN)).astype(BF)

        pl.loop(0, batch * seq // mc)(rows_step)
        y_copy(j).start()

    pl.loop(0, n_tiles)(tile)
    y_copy(n_tiles - 2).wait()
    y_copy(n_tiles - 1).wait()


def solution(mesh):
    dma = pltpu.SemaphoreType.DMA

    def local_block(hidden, positions, norm_gain, w_query, w_key, w_value, w_out):
        batch, seq, dim = hidden.shape
        heads = w_out.shape[0]
        n_kv = w_key.shape[1] // HD
        first = batch // 2
        nb = 2
        n_chunks = batch // nb
        freq = (10000.0 ** (-2.0 * np.arange(HD // 2, dtype=np.float64) / HD)).astype(np.float32)
        freq = jnp.asarray(np.concatenate([freq, freq])[None, :])
        hbm = pl.BlockSpec(memory_space=pl.ANY)
        vmem = pl.BlockSpec(memory_space=pltpu.VMEM)
        kv_shape = (batch, 2 * n_kv, seq, HD)
        blk = (2 * n_kv, seq, HD)
        shape = jax.ShapeDtypeStruct
        forward_q = ((1, 0), (2, 1), (3, 2), (5, 3), (6, 4))
        forward_a = ((1, 5), (4, 6))
        q, o_first, own, r1, r2, r3 = pl.pallas_call(
            functools.partial(front_kernel, n_kv, first, forward_q, forward_a),
            in_specs=[hbm, vmem, vmem, vmem, hbm, hbm, hbm],
            out_specs=[hbm] * 6,
            out_shape=[
                shape((batch, heads, seq, HD), BF), shape((first * seq, heads * HD), BF),
                shape((batch - first,) + blk, BF), shape(kv_shape, BF), shape(kv_shape, BF), shape(kv_shape, BF)],
            scratch_shapes=[
                pltpu.VMEM(((batch + nb) * seq, dim), BF), pltpu.VMEM((nb * seq, dim), BF), pltpu.VMEM((nb * seq, dim), BF), pltpu.VMEM(kv_shape, BF),
                pltpu.VMEM((batch * seq, HD), F32), pltpu.VMEM((batch * seq, HD), F32),
                pltpu.VMEM((2, nb, seq, dim), BF), pltpu.VMEM((3, dim, TN), BF),
                pltpu.VMEM((3, batch, TN // HD, seq, HD), BF), pltpu.VMEM((2, 512, TN), F32),
                pltpu.VMEM((2, heads, seq, HD), BF), pltpu.VMEM((2, 3) + blk, BF), pltpu.VMEM((2, seq, heads * HD), BF),
                dma((2,)), dma((3,)), dma((3,)), dma((2,)), dma((2, 3)), dma((2,)), dma,
            ] + [dma((n_chunks,))] * 6,
            compiler_params=pltpu.CompilerParams(vmem_limit_bytes=VMEM_LIMIT, collective_id=0, has_side_effects=True),
            cost_estimate=pl.CostEstimate(flops=2 * batch * seq * dim * (heads + 2 * n_kv) * HD, bytes_accessed=10 * batch * seq * dim, transcendentals=0),
            name="front",
        )(hidden, positions, norm_gain.reshape(dim // HD, HD), freq, w_query, w_key, w_value)
        half = batch - first
        return pl.pallas_call(
            functools.partial(back_kernel, n_kv, first),
            in_specs=[hbm] * 8, out_specs=hbm,
            out_shape=shape((batch, seq, dim), BF),
            scratch_shapes=[
                pltpu.VMEM((batch * seq, heads * HD), BF), pltpu.VMEM((2, heads * HD, TN), BF),
                pltpu.VMEM((2, batch, seq, TN), BF), pltpu.VMEM((2, batch, seq, TN), BF),
                pltpu.VMEM((2, heads, seq, HD), BF), pltpu.VMEM((2, 4) + blk, BF),
                dma, dma((2,)), dma((2,)), dma((2,)), dma((2,)), dma((2, 4)),
            ],
            compiler_params=pltpu.CompilerParams(vmem_limit_bytes=VMEM_LIMIT),
            cost_estimate=pl.CostEstimate(flops=2 * batch * seq * dim * heads * HD, bytes_accessed=10 * batch * seq * dim, transcendentals=0),
            name="back",
        )(q, o_first, own, r1, r2, r3, w_out.reshape(heads * HD, dim), hidden)

    act_spec = P('dp', 'cp', None)
    return jax.shard_map(local_block, mesh=mesh, in_specs=(act_spec, P('dp', 'cp'), P(), P(), P(), P(), P()), out_specs=act_spec, check_vma=False)
```
